32 devices in a mesh: ch: 16 (over z, x, core), rep: 2 (over y).
Axes of the slice: x: 2, y: 2, z: 4, core: 2. Of those that a mesh axis runs over, the one named last changes fastest.
Arguments:
- fields_a: bfloat16 [32, 128, 4096], P('rep', 'ch'), parts along dimension 0, may hold values from -6 to 6
- latent_b: bfloat16 [32, 2048, 512], P('rep', 'ch'), parts along dimension 0, may hold values from -6 to 6
- regrid_w: bfloat16 [32, 1, 128, 64], replicated, may hold values from -0.5 to 0.5
- cell_tiles: int32 [32, 1], replicated, may hold values from 0 to 31, as said below
- norm_a: float32 [128], replicated, may hold values from 0.5 to 1.5
- enc_in: bfloat16 [128, 512], replicated, may hold values from -0.5 to 0.5
- enc_mid: bfloat16 [512, 512], replicated, may hold values from -0.25 to 0.25
- enc_out: bfloat16 [512, 512], replicated, may hold values from -0.25 to 0.25
- norm_b: float32 [512], replicated, may hold values from 0.5 to 1.5
- dec_mid: bfloat16 [512, 512], replicated, may hold values from -0.25 to 0.25
- dec_out: bfloat16 [512, 128], replicated, may hold values from -0.25 to 0.25
Outputs:
- latent_a: bfloat16 [32, 2048, 512], P('rep', 'ch'), parts along dimension 0
- cells_b: bfloat16 [32, 128, 4096], P('rep', 'ch'), parts along dimension 0
The draws below stay inside these ranges and needn't reach their ends.
There are 2 independent parts, one for each index of `rep`. The reference program is written for one: setup_inputs(seed, part) draws one part's arguments, and reference() takes and returns one part's arrays. A program takes and returns all parts, laid end to end along the dimension named above; an argument that names none is the same for every part. Nothing has to cross between parts.
Inputs may be any that keep to these rules, and one draw needn't show every extreme that they name: The one column of cell_tiles names every one of the 32 cell blocks exactly once.
All inputs are finite; a program needn't handle non-finite values.
Results may differ from the reference program's by a relative error of at most 0.0066.
Values may be sent and summed in bfloat16 or wider, within the bound.
A program may use at most 64 MiB of HBM per device.

```python
import jax
import jax.numpy as jnp
from jax import lax

CHANNELS = 128
HIDDEN_SIZE = 512
ENS = 16
BN = 64
BC = 128
K = 1
NODES = 2048
NB = 32
CELLS = 4096


def draw_cell_tiles(key, part):
    columns = [jax.random.permutation(jax.random.fold_in(key, 11 + column), NB) for column in range(K)]
    return jnp.stack(columns, axis=1).astype(jnp.int32)


def block_scale(key, extent, cuts, least, largest):
    loudness, own = 1.0, jax.random.fold_in(key, 6)
    for position, blocks in cuts:
        heights = jnp.exp(jax.random.uniform(jax.random.fold_in(own, position), (blocks,), jnp.float32, least / len(cuts), largest / len(cuts)))
        loudness = loudness * jnp.repeat(heights, extent[position] // blocks).reshape([-1 if axis == position else 1 for axis in range(len(extent))])
    return loudness


def normal_values(key, dims, scale, limit, cuts=(), kind=jnp.bfloat16):
    result = scale * jax.random.normal(key, dims, jnp.float32)
    if cuts:
        result = result * block_scale(key, dims, cuts, -0.22, 0.18)
    return jnp.clip(result, -limit, limit).astype(kind)


def setup_inputs(seed: int = 0, part: int = 0) -> dict:
    seeds = jax.random.split(jax.random.key(seed), 12)
    own_keys = jax.random.split(jax.random.fold_in(seeds[11], part), 12)
    return {
        "fields_a": normal_values(own_keys[0], (ENS, CHANNELS, CELLS), 1.0, 6.0, ((1, 16),)),
        "latent_b": normal_values(own_keys[1], (ENS, NODES, HIDDEN_SIZE), 1.0, 6.0, ((1, 16),)),
        "regrid_w": normal_values(seeds[2], (NB, K, BC, BN), (K * BC) ** -0.5, 0.5),
        "cell_tiles": draw_cell_tiles(jax.random.fold_in(seeds[11], 71), part),
        "norm_a": jnp.clip(1.0 + 0.1 * jax.random.normal(seeds[4], (CHANNELS,), jnp.float32), 0.5, 1.5),
        "enc_in": normal_values(seeds[5], (CHANNELS, HIDDEN_SIZE), CHANNELS ** -0.5, 0.5),
        "enc_mid": normal_values(seeds[6], (HIDDEN_SIZE, HIDDEN_SIZE), HIDDEN_SIZE ** -0.5, 0.25),
        "enc_out": normal_values(seeds[7], (HIDDEN_SIZE, HIDDEN_SIZE), HIDDEN_SIZE ** -0.5, 0.25),
        "norm_b": jnp.clip(1.0 + 0.1 * jax.random.normal(seeds[8], (HIDDEN_SIZE,), jnp.float32), 0.5, 1.5),
        "dec_mid": normal_values(seeds[9], (HIDDEN_SIZE, HIDDEN_SIZE), HIDDEN_SIZE ** -0.5, 0.25),
        "dec_out": normal_values(seeds[10], (HIDDEN_SIZE, CHANNELS), HIDDEN_SIZE ** -0.5, 0.25),
    }


EPSILON = 1e-05

def normalize(values, gain_vec, along):
    average = lax.optimization_barrier(jnp.mean(values, axis=along, keepdims=True))
    centred = values - average
    spread = lax.optimization_barrier(jnp.mean(centred * centred, axis=along, keepdims=True))
    return centred * lax.rsqrt(spread + EPSILON) * gain_vec

def reference(fields_a, latent_b, regrid_w, cell_tiles, norm_a, enc_in, enc_mid, enc_out, norm_b, dec_mid, dec_out):
    blocks = fields_a.reshape(ENS, CHANNELS, NB, BC)
    chosen = jnp.take(blocks, cell_tiles, axis=2).reshape(ENS, CHANNELS, NB, K * BC)
    weights = regrid_w.reshape(NB, K * BC, BN)
    grid_a = jnp.einsum('ecnj,njm->ecnm', chosen.astype(jnp.float32), weights.astype(jnp.float32), precision=lax.Precision.HIGHEST).astype(jnp.bfloat16)
    grid_a = grid_a.reshape(ENS, CHANNELS, NODES)

    def encode_one(grid_one):
        values = grid_one.T.astype(jnp.float32)
        normed = normalize(values, norm_a, -1).astype(jnp.bfloat16)
        base = jnp.dot(normed, enc_in, preferred_element_type=jnp.float32).astype(jnp.bfloat16)
        middle = jax.nn.silu(jnp.dot(base, enc_mid, preferred_element_type=jnp.float32)).astype(jnp.bfloat16)
        return (base.astype(jnp.float32) + jnp.dot(middle, enc_out, preferred_element_type=jnp.float32)).astype(jnp.bfloat16)
    latent_a = lax.map(encode_one, grid_a)

    def decode_one(latent_one):
        normed = normalize(latent_one.astype(jnp.float32), norm_b, -1).astype(jnp.bfloat16)
        middle = jax.nn.silu(jnp.dot(normed, dec_mid, preferred_element_type=jnp.float32)).astype(jnp.bfloat16)
        return jnp.dot(middle, dec_out, preferred_element_type=jnp.float32).astype(jnp.bfloat16)
    nodes_b = lax.map(decode_one, latent_b)
    node_blocks = jnp.transpose(nodes_b, (0, 2, 1)).reshape(ENS, CHANNELS, NB, BN)
    inverse = jnp.argsort(cell_tiles, axis=0).astype(jnp.int32).T
    picked = jnp.take(node_blocks, inverse, axis=2)
    weight_sel = regrid_w[inverse, jnp.arange(K).astype(jnp.int32)[:, None]]
    total = jnp.einsum('ecknm,knbm->ecnb', picked.astype(jnp.float32), weight_sel.astype(jnp.float32), precision=lax.Precision.HIGHEST)
    cells_b = total.astype(jnp.bfloat16).reshape(ENS, CHANNELS, CELLS)
    return (latent_a, cells_b)
```

```python
import functools

import jax
import jax.numpy as jnp
from jax import lax
from jax.experimental import pallas as pl
from jax.experimental.pallas import tpu as pltpu
from jax.sharding import PartitionSpec as P

EPSILON = 1e-05
F32, BF16 = jnp.float32, jnp.bfloat16


def partner(me, step, count):
    if count & (count - 1):
        return lax.rem(me + step, count)
    result, bit = 0, 1
    while bit < count:
        mine, flip = lax.rem(me // bit, 2), lax.rem(step // bit, 2)
        result = result + (mine + flip - 2 * mine * flip) * bit
        bit *= 2
    return result


def silu(values):
    half = 0.5 * values
    return half + half * jnp.tanh(half)


def dot(left, right):
    return jnp.dot(left, right, preferred_element_type=F32)


def kernel(
    groups, samples, pieces,
    tiles, inverse,
    fields_h, latent_h, regrid_h, norm_a_h, enc_in_h, enc_mid_h, enc_out_h, norm_b_h, dec_mid_h, dec_out_h,
    latent_o, cells_o,
    fields, latent, regrid, norm_a, enc_in, enc_mid, enc_out, norm_b, dec_mid, dec_out,
    diag, send_a, recv_a, send_b, recv_b, mixed, latent_v, cells_v,
    in_sems, out_sems, send_sems, recv_sems,
):
    me = lax.axis_index("ch")
    rows, nodes = recv_a.shape[1], recv_a.shape[2]
    own = rows // samples
    bn, bc = regrid.shape[1], regrid.shape[2]
    per = nodes // bn
    blocks = regrid.shape[0]
    each = samples // pieces
    part = each * own

    loads = [
        pltpu.make_async_copy(src, dst, in_sems.at[i + 1])
        for i, (src, dst) in enumerate(
            [
                (regrid_h, regrid), (latent_h, latent), (norm_b_h, norm_b),
                (dec_mid_h, dec_mid), (dec_out_h, dec_out), (norm_a_h, norm_a), (enc_in_h, enc_in),
                (enc_mid_h, enc_mid), (enc_out_h, enc_out),
            ]
        )
    ]
    loads[0].start()

    @pl.loop(0, blocks)
    def _(block):
        pltpu.make_async_copy(
            fields_h.at[:, pl.ds(pl.multiple_of(block * bc, bc), bc)], fields.at[block], in_sems.at[0]
        ).start()

    for load in loads[1:]:
        load.start()

    barrier = pltpu.get_barrier_semaphore()

    @pl.loop(1, groups)
    def _(step):
        pl.semaphore_signal(
            barrier, inc=1, device_id={"ch": partner(me, step, groups)},
            device_id_type=pl.DeviceIdType.MESH,
        )

    def wait_all(ref, sem):
        pltpu.make_async_copy(ref, ref, sem).wait()

    wait_all(fields, in_sems.at[0])
    loads[0].wait()

    def regrid_to(owner):
        lines = []
        for k in range(per):
            sides = [jnp.zeros((bn, bc), BF16)] * per
            sides[k] = regrid[owner * per + k]
            lines.append(jnp.concatenate(sides, axis=1))
        weights = jnp.concatenate(lines, axis=0)
        diag[owner] = weights
        chosen = jnp.concatenate(
            [fields[tiles[owner * per + k]] for k in range(per)], axis=1
        )
        return lax.dot_general(
            chosen, weights, (((1,), (1,)), ((), ())), preferred_element_type=F32
        ).astype(BF16)

    recv_a[me] = regrid_to(me)

    @pl.loop(1, groups)
    def _(step):
        owner = partner(me, step, groups)
        send_a[owner] = regrid_to(owner)

    pl.semaphore_wait(barrier, groups - 1)

    @pl.loop(1, groups)
    def _(step):
        owner = partner(me, groups - step, groups)
        pltpu.make_async_remote_copy(
            src_ref=send_a.at[owner], dst_ref=recv_a.at[me],
            send_sem=send_sems.at[0], recv_sem=recv_sems.at[0],
            device_id={"ch": owner}, device_id_type=pl.DeviceIdType.MESH,
        ).start()

    for i in range(1, 5):
        loads[i].wait()
    length = each * nodes

    def decode(piece):
        values = latent[pl.ds(pl.multiple_of(piece * length, length), length), :].astype(F32)
        centred = values - jnp.mean(values, axis=1, keepdims=True)
        spread = jnp.mean(centred * centred, axis=1, keepdims=True)
        normed = (centred * lax.rsqrt(spread + EPSILON) * norm_b[...]).astype(BF16)
        middle = silu(dot(normed, dec_mid[...])).astype(BF16)
        decoded = dot(middle, dec_out[...])
        turned = [
            decoded[e * nodes : (e + 1) * nodes].T.reshape(groups, own, nodes) for e in range(each)
        ]
        send_b[piece] = jnp.concatenate(turned, axis=1).astype(BF16)
        recv_b[piece, me] = send_b[piece, me]

    def send_piece(piece):
        @pl.loop(1, groups)
        def _(step):
            owner = partner(me, groups - step, groups)
            pltpu.make_async_remote_copy(
                src_ref=send_b.at[piece, owner], dst_ref=recv_b.at[piece, me],
                send_sem=send_sems.at[1 + piece], recv_sem=recv_sems.at[1 + piece],
                device_id={"ch": owner}, device_id_type=pl.DeviceIdType.MESH,
            ).start()

    decode(0)

    @pl.loop(1, pieces)
    def _(piece):
        decode(piece)
        send_piece(piece - 1)

    for i in range(5, 9):
        loads[i].wait()
    send_piece(pieces - 1)
    wait_all(recv_a.at[pl.ds(0, groups - 1)], recv_sems.at[0])

    def written(piece):
        span = pl.ds(pl.multiple_of(piece * length, length), length)
        return pltpu.make_async_copy(latent_v.at[span], latent_o.at[span], out_sems.at[piece])

    @pl.loop(0, pieces)
    def _(piece):
        values = recv_a[:, pl.ds(pl.multiple_of(piece * part, part), part), :].astype(F32)
        lines = []
        for e in range(each):
            one = values[:, e * own : (e + 1) * own].reshape(groups * own, nodes)
            centred = one - jnp.mean(one, axis=0, keepdims=True)
            spread = jnp.mean(centred * centred, axis=0, keepdims=True)
            scaled = centred * lax.rsqrt(spread + EPSILON)
            lines.append((scaled.T * norm_a[...]).astype(BF16))
        base = dot(jnp.concatenate(lines, axis=0), enc_in[...]).astype(BF16)
        middle = silu(dot(base, enc_mid[...])).astype(BF16)
        result = base.astype(F32) + dot(middle, enc_out[...])
        latent_v[pl.ds(pl.multiple_of(piece * length, length), length), :] = result.astype(BF16)
        written(piece).start()

    for piece in range(pieces):
        wait_all(recv_b.at[piece, pl.ds(0, groups - 1)], recv_sems.at[1 + piece])

        @pl.loop(0, groups, unroll=groups <= 16)
        def _(owner):
            total = dot(recv_b[piece, owner], diag[owner]).astype(BF16)
            for k in range(per):
                mixed[owner * per + k] = total[:, k * bc : (k + 1) * bc]

        span = pl.ds(piece * part, part)

        @pl.loop(0, blocks, unroll=blocks <= 32)
        def _(block):
            cells_v[span, pl.ds(pl.multiple_of(block * bc, bc), bc)] = mixed[inverse[block]]

        pltpu.make_async_copy(cells_v.at[span], cells_o.at[span], out_sems.at[pieces + piece]).start()

    for piece in range(pieces):
        span = pl.ds(piece * part, part)
        pltpu.make_async_copy(cells_v.at[span], cells_o.at[span], out_sems.at[pieces + piece]).wait()
        written(piece).wait()
        wait_all(send_b.at[piece, pl.ds(0, groups - 1)], send_sems.at[1 + piece])
    wait_all(send_a.at[pl.ds(0, groups - 1)], send_sems.at[0])


def shards(
    fields_a, latent_b, regrid_w, cell_tiles, norm_a, enc_in, enc_mid, enc_out, norm_b, dec_mid, dec_out
):
    groups = lax.axis_size("ch")
    samples, own, cells = fields_a.shape
    nodes, hidden = latent_b.shape[1:]
    blocks, reads, bc, bn = regrid_w.shape
    assert reads == 1 and blocks % groups == 0 and nodes * groups == blocks * bn
    per = blocks // groups
    rows = samples * own
    pieces = max(p for p in (1, 2, 4) if samples % p == 0 and (rows // p) % 16 == 0)

    tiles = cell_tiles.reshape(blocks)
    order = jnp.arange(blocks, dtype=jnp.int32)
    inverse = jnp.sum(jnp.where(tiles[None, :] == order[:, None], order[None, :], 0), axis=1)
    operands = (
        fields_a.reshape(rows, cells),
        latent_b.reshape(samples * nodes, hidden),
        jnp.swapaxes(regrid_w.reshape(blocks, bc, bn), 1, 2),
        norm_a.reshape(1, -1), enc_in, enc_mid, enc_out,
        norm_b.reshape(1, -1), dec_mid, dec_out,
    )
    smem, anywhere = pl.BlockSpec(memory_space=pltpu.SMEM), pl.BlockSpec(memory_space=pl.ANY)
    latent_a, cells_b = pl.pallas_call(
        functools.partial(kernel, groups, samples, pieces),
        out_shape=(
            jax.ShapeDtypeStruct((samples * nodes, hidden), BF16),
            jax.ShapeDtypeStruct((rows, cells), BF16),
        ),
        in_specs=[smem, smem] + [anywhere] * len(operands),
        out_specs=(anywhere, anywhere),
        scratch_shapes=[pltpu.VMEM((blocks, rows, bc), BF16)]
        + [pltpu.VMEM(x.shape, x.dtype) for x in operands[1:]]
        + [
            pltpu.VMEM((groups, nodes, per * bc), BF16),
            pltpu.VMEM((groups, rows, nodes), BF16),
            pltpu.VMEM((groups, rows, nodes), BF16),
            pltpu.VMEM((pieces, groups, rows // pieces, nodes), BF16),
            pltpu.VMEM((pieces, groups, rows // pieces, nodes), BF16),
            pltpu.VMEM((blocks, rows // pieces, bc), BF16),
            pltpu.VMEM((samples * nodes, hidden), BF16),
            pltpu.VMEM((rows, cells), BF16),
            pltpu.SemaphoreType.DMA((len(operands),)),
            pltpu.SemaphoreType.DMA((2 * pieces,)),
            pltpu.SemaphoreType.DMA((1 + pieces,)),
            pltpu.SemaphoreType.DMA((1 + pieces,)),
        ],
        compiler_params=pltpu.CompilerParams(
            collective_id=0, has_side_effects=True, vmem_limit_bytes=60 * 2**20
        ),
    )(tiles, inverse, *operands)
    return latent_a.reshape(samples, nodes, hidden), cells_b.reshape(samples, own, cells)


def solution(mesh):
    split = P("rep", "ch", None)
    return jax.shard_map(
        shards,
        mesh=mesh,
        in_specs=(split, split) + (P(),) * 9,
        out_specs=(split, split),
        check_vma=False,
    )
```

```python
import functools

import jax
import jax.numpy as jnp
from jax import lax
from jax.experimental import pallas as pl
from jax.experimental.pallas import tpu as pltpu
from jax.sharding import PartitionSpec as P

EPSILON = 1e-05
VMEM_BYTES = 67043328
F32, BF16 = jnp.float32, jnp.bfloat16


def partner(me, step, count):
    if count & (count - 1):
        return lax.rem(me + step, count)
    result, bit = 0, 1
    while bit < count:
        mine, flip = lax.rem(me // bit, 2), lax.rem(step // bit, 2)
        result = result + (mine + flip - 2 * mine * flip) * bit
        bit *= 2
    return result


def silu(values):
    half = 0.5 * values
    return half + half * jnp.tanh(half)


def dot(left, right):
    return jnp.dot(left, right, preferred_element_type=F32)


def kernel(
    groups, samples, pieces,
    tiles, tiles_h,
    fields_h, latent_h, regrid_h, norm_a_h, enc_in_h, enc_mid_h, enc_out_h, norm_b_h, dec_mid_h, dec_out_h,
    latent_v, mixed, tiles_v,
    fields, latent, regrid, norm_a, enc_in, enc_mid, enc_out, norm_b, dec_mid, dec_out,
    diag, send_a, recv_a, send_b, recv_b,
    in_sems, send_sems, recv_sems,
):
    me = lax.axis_index("ch")
    rows, nodes = recv_a.shape[1], recv_a.shape[2]
    own = rows // samples
    bn, bc = regrid.shape[1], regrid.shape[2]
    per = nodes // bn
    blocks = regrid.shape[0]
    each = samples // pieces
    part = each * own

    loads = [
        pltpu.make_async_copy(src, dst, in_sems.at[i + 1])
        for i, (src, dst) in enumerate(
            [
                (regrid_h, regrid), (latent_h, latent), (norm_b_h, norm_b),
                (dec_mid_h, dec_mid), (dec_out_h, dec_out), (norm_a_h, norm_a), (enc_in_h, enc_in),
                (enc_mid_h, enc_mid), (enc_out_h, enc_out), (tiles_h, tiles_v),
            ]
        )
    ]
    loads[0].start()

    @pl.loop(0, blocks)
    def _(block):
        pltpu.make_async_copy(
            fields_h.at[:, pl.ds(pl.multiple_of(block * bc, bc), bc)], fields.at[block], in_sems.at[0]
        ).start()

    for load in loads[1:]:
        load.start()

    barrier = pltpu.get_barrier_semaphore()

    @pl.loop(1, groups)
    def _(step):
        pl.semaphore_signal(
            barrier, inc=1, device_id={"ch": partner(me, step, groups)},
            device_id_type=pl.DeviceIdType.MESH,
        )

    def wait_all(ref, sem):
        pltpu.make_async_copy(ref, ref, sem).wait()

    wait_all(fields, in_sems.at[0])
    loads[0].wait()

    def regrid_to(owner):
        lines = []
        for k in range(per):
            sides = [jnp.zeros((bn, bc), BF16)] * per
            sides[k] = regrid[owner * per + k]
            lines.append(jnp.concatenate(sides, axis=1))
        weights = jnp.concatenate(lines, axis=0)
        diag[owner] = weights
        chosen = jnp.concatenate(
            [fields[tiles[owner * per + k]] for k in range(per)], axis=1
        )
        return lax.dot_general(
            chosen, weights, (((1,), (1,)), ((), ())), preferred_element_type=F32
        ).astype(BF16)

    recv_a[me] = regrid_to(me)

    @pl.loop(1, groups)
    def _(step):
        owner = partner(me, step, groups)
        send_a[owner] = regrid_to(owner)

    pl.semaphore_wait(barrier, groups - 1)

    @pl.loop(1, groups)
    def _(step):
        owner = partner(me, groups - step, groups)
        pltpu.make_async_remote_copy(
            src_ref=send_a.at[owner], dst_ref=recv_a.at[me],
            send_sem=send_sems.at[0], recv_sem=recv_sems.at[0],
            device_id={"ch": owner}, device_id_type=pl.DeviceIdType.MESH,
        ).start()

    for i in range(1, 5):
        loads[i].wait()
    length = each * nodes

    def decode(piece):
        values = latent[pl.ds(pl.multiple_of(piece * length, length), length), :].astype(F32)
        centred = values - jnp.mean(values, axis=1, keepdims=True)
        spread = jnp.mean(centred * centred, axis=1, keepdims=True)
        normed = (centred * lax.rsqrt(spread + EPSILON) * norm_b[...]).astype(BF16)
        middle = silu(dot(normed, dec_mid[...])).astype(BF16)
        decoded = dot(middle, dec_out[...])
        turned = [
            decoded[e * nodes : (e + 1) * nodes].T.reshape(groups, own, nodes) for e in range(each)
        ]
        send_b[piece] = jnp.concatenate(turned, axis=1).astype(BF16)
        recv_b[piece, me] = send_b[piece, me]

    def send_piece(piece):
        @pl.loop(1, groups)
        def _(step):
            owner = partner(me, groups - step, groups)
            pltpu.make_async_remote_copy(
                src_ref=send_b.at[piece, owner], dst_ref=recv_b.at[piece, me],
                send_sem=send_sems.at[1 + piece], recv_sem=recv_sems.at[1 + piece],
                device_id={"ch": owner}, device_id_type=pl.DeviceIdType.MESH,
            ).start()

    decode(0)

    @pl.loop(1, pieces)
    def _(piece):
        decode(piece)
        send_piece(piece - 1)

    for i in range(5, 10):
        loads[i].wait()
    send_piece(pieces - 1)
    wait_all(recv_a.at[pl.ds(0, groups - 1)], recv_sems.at[0])

    @pl.loop(0, pieces)
    def _(piece):
        values = recv_a[:, pl.ds(pl.multiple_of(piece * part, part), part), :].astype(F32)
        lines = []
        for e in range(each):
            one = values[:, e * own : (e + 1) * own].reshape(groups * own, nodes)
            centred = one - jnp.mean(one, axis=0, keepdims=True)
            spread = jnp.mean(centred * centred, axis=0, keepdims=True)
            scaled = centred * lax.rsqrt(spread + EPSILON)
            lines.append((scaled.T * norm_a[...]).astype(BF16))
        base = dot(jnp.concatenate(lines, axis=0), enc_in[...]).astype(BF16)
        middle = silu(dot(base, enc_mid[...])).astype(BF16)
        result = base.astype(F32) + dot(middle, enc_out[...])
        latent_v[pl.ds(pl.multiple_of(piece * length, length), length), :] = result.astype(BF16)

    for piece in range(pieces):
        wait_all(recv_b.at[piece, pl.ds(0, groups - 1)], recv_sems.at[1 + piece])

        @pl.loop(0, groups, unroll=groups <= 16)
        def _(owner):
            total = dot(recv_b[piece, owner], diag[owner]).astype(BF16)
            for k in range(per):
                mixed[owner * per + k, pl.ds(piece * part, part), :] = total[:, k * bc : (k + 1) * bc]

    for piece in range(pieces):
        wait_all(send_b.at[piece, pl.ds(0, groups - 1)], send_sems.at[1 + piece])
    wait_all(send_a.at[pl.ds(0, groups - 1)], send_sems.at[0])


def place(tiles_h, latent_v, mixed, latent_o, cells_o, tiles, sems):
    blocks, _, bc = mixed.shape
    fetch = pltpu.make_async_copy(tiles_h, tiles, sems.at[2])
    fetch.start()
    copy = pltpu.make_async_copy(latent_v, latent_o, sems.at[0])
    copy.start()
    fetch.wait()

    @pl.loop(0, blocks, unroll=blocks <= 32)
    def _(block):
        pltpu.make_async_copy(
            mixed.at[block], cells_o.at[:, pl.ds(pl.multiple_of(tiles[0, block] * bc, bc), bc)], sems.at[1]
        ).start()

    pltpu.make_async_copy(mixed, mixed, sems.at[1]).wait()
    copy.wait()


def shards(
    fields_a, latent_b, regrid_w, cell_tiles, norm_a, enc_in, enc_mid, enc_out, norm_b, dec_mid, dec_out
):
    groups = lax.axis_size("ch")
    samples, own, cells = fields_a.shape
    nodes, hidden = latent_b.shape[1:]
    blocks, reads, bc, bn = regrid_w.shape
    assert reads == 1 and blocks % groups == 0 and nodes * groups == blocks * bn
    per = blocks // groups
    rows = samples * own
    pieces = max(p for p in (1, 2, 4) if samples % p == 0 and (rows // p) % 16 == 0)

    tiles = cell_tiles.reshape(blocks)
    operands = (
        fields_a.reshape(rows, cells),
        latent_b.reshape(samples * nodes, hidden),
        jnp.swapaxes(regrid_w.reshape(blocks, bc, bn), 1, 2),
        norm_a.reshape(1, -1), enc_in, enc_mid, enc_out,
        norm_b.reshape(1, -1), dec_mid, dec_out,
    )
    smem, vmem = pl.BlockSpec(memory_space=pltpu.SMEM), pl.BlockSpec(memory_space=pltpu.VMEM)
    hbm = pl.BlockSpec(memory_space=pltpu.HBM)
    latent_v, mixed, tiles_v = pl.pallas_call(
        functools.partial(kernel, groups, samples, pieces),
        out_shape=(
            pltpu.VMEM((samples * nodes, hidden), BF16),
            pltpu.VMEM((blocks, rows, bc), BF16),
            pltpu.VMEM((1, blocks), jnp.int32),
        ),
        in_specs=[smem, hbm] + [hbm] * len(operands),
        out_specs=(vmem, vmem, vmem),
        scratch_shapes=[pltpu.VMEM((blocks, rows, bc), BF16)]
        + [pltpu.VMEM(x.shape, x.dtype) for x in operands[1:]]
        + [
            pltpu.VMEM((groups, nodes, per * bc), BF16),
            pltpu.VMEM((groups, rows, nodes), BF16),
            pltpu.VMEM((groups, rows, nodes), BF16),
            pltpu.VMEM((pieces, groups, rows // pieces, nodes), BF16),
            pltpu.VMEM((pieces, groups, rows // pieces, nodes), BF16),
            pltpu.SemaphoreType.DMA((len(operands) + 1,)),
            pltpu.SemaphoreType.DMA((1 + pieces,)),
            pltpu.SemaphoreType.DMA((1 + pieces,)),
        ],
        compiler_params=pltpu.CompilerParams(
            collective_id=0, has_side_effects=True, vmem_limit_bytes=VMEM_BYTES - 2 * (samples * nodes * hidden + rows * cells) - 2**14
        ),
    )(tiles, tiles.reshape(1, blocks), *operands)
    latent_a, cells_b = pl.pallas_call(
        place,
        out_shape=(
            jax.ShapeDtypeStruct((samples * nodes, hidden), BF16),
            jax.ShapeDtypeStruct((rows, cells), BF16),
        ),
        in_specs=[vmem, vmem, vmem],
        out_specs=(hbm, hbm),
        scratch_shapes=[pltpu.SMEM((1, blocks), jnp.int32), pltpu.SemaphoreType.DMA((3,))],
        compiler_params=pltpu.CompilerParams(vmem_limit_bytes=16 * 2**20),
    )(tiles_v, latent_v, mixed)
    return latent_a.reshape(samples, nodes, hidden), cells_b.reshape(samples, own, cells)


def solution(mesh):
    split = P("rep", "ch", None)
    return jax.shard_map(
        shards,
        mesh=mesh,
        in_specs=(split, split) + (P(),) * 9,
        out_specs=(split, split),
        check_vma=False,
    )
```
